32 devices in a mesh: rep: 2 (over x), dp: 16 (over y, z, core).
Axes of the slice: x: 2, y: 2, z: 4, core: 2. Of those that a mesh axis runs over, the one named last changes fastest.
Arguments:
- x: bfloat16 [32, 2048, 640], P(('rep', 'dp')), parts along dimension 0
- dy: bfloat16 [32, 2048, 640], P(('rep', 'dp')), parts along dimension 0
- wq: bfloat16 [2, 640, 640], P(None, 'dp')
- wk: bfloat16 [2, 640, 640], P(None, 'dp')
- wv: bfloat16 [2, 640, 640], P(None, 'dp')
- wo: bfloat16 [2, 640, 640], P(None, 'dp')
- w_gate: bfloat16 [2, 640, 2560], P(None, 'dp')
- w_up: bfloat16 [2, 640, 2560], P(None, 'dp')
- w_down: bfloat16 [2, 2560, 640], P(None, 'dp')
- m_wq: float32 [2, 640, 640], P(None, 'dp')
- m_wk: float32 [2, 640, 640], P(None, 'dp')
- m_wv: float32 [2, 640, 640], P(None, 'dp')
- m_wo: float32 [2, 640, 640], P(None, 'dp')
- m_w_gate: float32 [2, 640, 2560], P(None, 'dp')
- m_w_up: float32 [2, 640, 2560], P(None, 'dp')
- m_w_down: float32 [2, 2560, 640], P(None, 'dp')
- v_wq: float32 [2, 640, 640], P(None, 'dp')
- v_wk: float32 [2, 640, 640], P(None, 'dp')
- v_wv: float32 [2, 640, 640], P(None, 'dp')
- v_wo: float32 [2, 640, 640], P(None, 'dp')
- v_w_gate: float32 [2, 640, 2560], P(None, 'dp')
- v_w_up: float32 [2, 640, 2560], P(None, 'dp')
- v_w_down: float32 [2, 2560, 640], P(None, 'dp')
Outputs:
- output 1: bfloat16 [4, 640, 640], P('rep', 'dp'), parts along dimension 0
- output 2: bfloat16 [4, 640, 640], P('rep', 'dp'), parts along dimension 0
- output 3: bfloat16 [4, 640, 640], P('rep', 'dp'), parts along dimension 0
- output 4: bfloat16 [4, 640, 640], P('rep', 'dp'), parts along dimension 0
- output 5: bfloat16 [4, 640, 2560], P('rep', 'dp'), parts along dimension 0
- output 6: bfloat16 [4, 640, 2560], P('rep', 'dp'), parts along dimension 0
- output 7: bfloat16 [4, 2560, 640], P('rep', 'dp'), parts along dimension 0
- output 8: float32 [4, 640, 640], P('rep', 'dp'), parts along dimension 0
- output 9: float32 [4, 640, 640], P('rep', 'dp'), parts along dimension 0
- output 10: float32 [4, 640, 640], P('rep', 'dp'), parts along dimension 0
- output 11: float32 [4, 640, 640], P('rep', 'dp'), parts along dimension 0
- output 12: float32 [4, 640, 2560], P('rep', 'dp'), parts along dimension 0
- output 13: float32 [4, 640, 2560], P('rep', 'dp'), parts along dimension 0
- output 14: float32 [4, 2560, 640], P('rep', 'dp'), parts along dimension 0
- output 15: float32 [4, 640, 640], P('rep', 'dp'), parts along dimension 0
- output 16: float32 [4, 640, 640], P('rep', 'dp'), parts along dimension 0
- output 17: float32 [4, 640, 640], P('rep', 'dp'), parts along dimension 0
- output 18: float32 [4, 640, 640], P('rep', 'dp'), parts along dimension 0
- output 19: float32 [4, 640, 2560], P('rep', 'dp'), parts along dimension 0
- output 20: float32 [4, 640, 2560], P('rep', 'dp'), parts along dimension 0
- output 21: float32 [4, 2560, 640], P('rep', 'dp'), parts along dimension 0
There are 2 independent parts. The reference program is written for one: setup_inputs(seed, part) draws one part's arguments, and reference() takes and returns one part's arrays. A program takes and returns all parts, laid end to end along the dimension named above; an argument that names none is the same for every part.
All inputs are finite; a program needn't handle non-finite values.
Results may differ from the reference program's by a relative error of at most 0.024.
Values are sent between devices in bfloat16 or wider.
A program may use at most 2 GiB of HBM per device.

```python
import jax
import jax.numpy as jnp
from jax import lax

SEQUENCES = 16
TOKENS = 2048
D = 640
HEADS = 5
KV_HEADS = 5
HEAD = 128
FF = 2560
LAYERS = 2
THETA = 10000
NAMES = ("wq", "wk", "wv", "wo", "w_gate", "w_up", "w_down")
SHAPES = {
    "wq": (LAYERS, D, HEADS * HEAD),
    "wk": (LAYERS, D, KV_HEADS * HEAD),
    "wv": (LAYERS, D, KV_HEADS * HEAD),
    "wo": (LAYERS, HEADS * HEAD, D),
    "w_gate": (LAYERS, D, FF),
    "w_up": (LAYERS, D, FF),
    "w_down": (LAYERS, FF, D),
}


def bump(key, n, height):
    away = (jnp.arange(n, dtype=jnp.int32) - jax.random.randint(key, (), 0, n, jnp.int32)) % n
    return jnp.where(away < n // 8, height, 1.0)


def together(key, own, strength):
    shared = jax.random.normal(key, own.shape[1:], jnp.float32)
    return (own + strength * shared) * lax.rsqrt(1 + strength * strength)


def setup_inputs(seed: int = 0, part: int = 0) -> dict:
    kx, kdy, ka, kb, kz, kf, kh, kl, *keys = jax.random.split(jax.random.key(seed), 8 + 3 * len(NAMES))
    kx, kdy, ka, kb = (jax.random.fold_in(k, part) for k in (kx, kdy, ka, kb))
    kw, km, kv = (keys[i::3] for i in range(3))
    shape = (SEQUENCES, TOKENS, D)
    much_x, much_dy = jax.random.uniform(kz, (2,), jnp.float32, 0.0, 1.0)
    loud = 2.0 ** jax.random.uniform(jax.random.fold_in(kz, 1), (), jnp.float32, -1.0, 2.0)
    layers = 2.0 ** jax.random.uniform(kl, (LAYERS, 1, 1), jnp.float32, -1.0, 1.0)
    times = {"wq": 1.0, "wk": 1.0, "wv": 2.0, "wo": layers, "w_gate": 1.0, "w_up": bump(kh, FF, 4.0), "w_down": layers}
    x = together(ka, jax.random.normal(kx, shape, jnp.float32), much_x) * bump(kf, D, 4.0)
    dy = together(kb, jax.random.normal(kdy, shape, jnp.float32), much_dy)
    drawn = {"x": x.astype(jnp.bfloat16), "dy": (loud * dy * (SEQUENCES * TOKENS) ** -0.5).astype(jnp.bfloat16)}
    for key, name in zip(kw, NAMES, strict=True):
        drawn[name] = (jax.random.normal(key, SHAPES[name], jnp.float32) * SHAPES[name][1] ** -0.5 * times[name]).astype(jnp.bfloat16)
    for key, name in zip(km, NAMES, strict=True):
        drawn[f"m_{name}"] = 0.1 * jax.random.normal(key, SHAPES[name], jnp.float32)
    for key, name in zip(kv, NAMES, strict=True):
        drawn[f"v_{name}"] = jax.random.uniform(key, SHAPES[name], jnp.float32, 0.02, 0.06)
    return drawn


def matmul(a, w):
    return jnp.dot(a, w, preferred_element_type=jnp.float32).astype(jnp.bfloat16)


def normed(h):
    wide = h.astype(jnp.float32)
    scale = lax.rsqrt(jnp.mean(wide**2, -1, keepdims=True) + 1e-6)
    return (wide * scale).astype(jnp.bfloat16)


def turned(t, theta):
    half = t.shape[-1] // 2
    angle = jnp.arange(t.shape[0], dtype=jnp.float32)[:, None] * theta ** (-jnp.arange(half, dtype=jnp.float32) / half)
    cos, sin = jnp.cos(angle)[:, None], jnp.sin(angle)[:, None]
    a, b = t[..., :half].astype(jnp.float32), t[..., half:].astype(jnp.float32)
    return jnp.concatenate([a * cos - b * sin, b * cos + a * sin], -1).astype(jnp.bfloat16)


def seen_by(q, k, v):
    tokens, kv = q.shape[0], k.shape[1]
    q = q.reshape(tokens, kv, -1, q.shape[-1])
    scores = jnp.einsum("tgsd,ugd->gstu", q.astype(jnp.float32), k.astype(jnp.float32)) * q.shape[-1] ** -0.5
    place = jnp.arange(tokens)
    weights = jax.nn.softmax(jnp.where(place[:, None] >= place, scores, -jnp.inf), -1).astype(jnp.bfloat16)
    return jnp.einsum("gstu,ugd->tgsd", weights.astype(jnp.float32), v.astype(jnp.float32)).astype(jnp.bfloat16).reshape(tokens, -1)


def layer(h, w):
    a = normed(h)
    q, k = (turned(matmul(a, w[name]).reshape(h.shape[0], -1, HEAD), THETA) for name in ("wq", "wk"))
    h = h + matmul(seen_by(q, k, matmul(a, w["wv"]).reshape(h.shape[0], -1, HEAD)), w["wo"])
    b = normed(h)
    gate = jnp.dot(b, w["w_gate"], preferred_element_type=jnp.float32)
    up = jnp.dot(b, w["w_up"], preferred_element_type=jnp.float32)
    return h + matmul((jax.nn.silu(gate) * up).astype(jnp.bfloat16), w["w_down"])


def adamw(w, m, v, g):
    m = 0.9 * m + 0.1 * g
    v = 0.95 * v + 0.05 * g * g
    step = m * lax.rsqrt(v + 1e-8) + 0.1 * w
    return (w - 0.02 * step).astype(jnp.bfloat16), m, v


def clipped(gradients, sum_of_squares, count):
    factor = jnp.minimum(1.0, 0.5 * lax.rsqrt(sum_of_squares / count + 1e-30))
    return [g * factor for g in gradients]


def stack(weights, h):
    return lax.scan(lambda h, w: (layer(h, w), None), h, weights)[0]


def reference(x, dy, wq, wk, wv, wo, w_gate, w_up, w_down, m_wq, m_wk, m_wv, m_wo, m_w_gate, m_w_up, m_w_down, v_wq, v_wk, v_wv, v_wo, v_w_gate, v_w_up, v_w_down):
    weights = dict(zip(NAMES, (wq, wk, wv, wo, w_gate, w_up, w_down), strict=True))

    def take(so_far, sequence):
        h, by_y = sequence
        _, back = jax.vjp(stack, weights, h)
        by_weights, by_h = back(by_y)
        return jax.tree.map(lambda total, term: total + term.astype(jnp.float32), so_far, by_weights), by_h

    none_yet = {name: jnp.zeros(w.shape, jnp.float32) for name, w in weights.items()}
    by_weights, by_x = lax.scan(take, none_yet, (x, dy))
    gradients = [by_weights[name].astype(jnp.bfloat16).astype(jnp.float32) for name in NAMES]
    gradients = clipped(gradients, sum(jnp.sum(g * g) for g in gradients), sum(g.size for g in gradients))
    first = (m_wq, m_wk, m_wv, m_wo, m_w_gate, m_w_up, m_w_down)
    second = (v_wq, v_wk, v_wv, v_wo, v_w_gate, v_w_up, v_w_down)
    new = [adamw(weights[name].astype(jnp.float32), m, v, g) for name, m, v, g in zip(NAMES, first, second, gradients, strict=True)]
    return tuple(one[which] for which in range(3) for one in new)
```

```python
import functools

import jax
import jax.numpy as jnp
from jax import lax
from jax.experimental import pallas as pl
from jax.experimental.pallas import tpu as pltpu
from jax.sharding import PartitionSpec as P


NEG = -1e30
HIDDEN = 2 * NEG
LOG2E = 1.4426950408889634
HEAD = 128
THETA = 10000
BF, F32 = jnp.bfloat16, jnp.float32
MiB = 2**20


def _dot(a, b, ca, cb):
    return lax.dot_general(a, b, (((ca,), (cb,)), ((), ())), preferred_element_type=F32)


def _params(limit, *axes):
    return pltpu.CompilerParams(dimension_semantics=axes, vmem_limit_bytes=limit * MiB)


def _cost(flops, size):
    return pl.CostEstimate(flops=int(flops), transcendentals=0, bytes_accessed=int(size))


def _normed(h):
    wide = h.astype(F32)
    scale = lax.rsqrt(jnp.mean(wide * wide, -1, keepdims=True) + 1e-6)
    return wide * scale, scale


def _norm_back(h, by_n):
    wide, by_n = h.astype(F32), by_n.astype(F32)
    scale = lax.rsqrt(jnp.mean(wide * wide, -1, keepdims=True) + 1e-6)
    inner = jnp.mean(by_n * wide, -1, keepdims=True)
    return (by_n * scale - wide * (scale * scale * scale * inner)).astype(BF)


def _heads(width):
    return [slice(i, i + HEAD) for i in range(0, width, HEAD)]


def _qkv_kernel(h_ref, wq_ref, wk_ref, wv_ref, cos_ref, sin_ref, out_ref):
    d = h_ref.shape[1]
    a = _normed(h_ref[...])[0].astype(BF)
    cos, sin = cos_ref[...], sin_ref[...]
    for n, w_ref in enumerate((wq_ref, wk_ref)):
        t = _dot(a, w_ref[...], 1, 0).astype(BF).astype(F32)
        for s in _heads(d):
            one = t[:, s]
            out_ref[:, n * d + s.start : n * d + s.stop] = (one * cos + pltpu.roll(one, HEAD // 2, 1) * sin).astype(BF)
    out_ref[:, 2 * d :] = _dot(a, wv_ref[...], 1, 0).astype(BF)


def qkv_forward(h, packed, at, cos, sin, tile=512):
    t, d = h.shape
    rows = lambda n: pl.BlockSpec((tile, n), lambda i: (i, 0))
    weight = lambda j: pl.BlockSpec((d, d), lambda i: (0, j))
    return pl.pallas_call(
        _qkv_kernel, grid=(t // tile,), name="qkv_forward",
        in_specs=[rows(d), weight(at), weight(at + 1), weight(at + 2), rows(HEAD), rows(HEAD)],
        out_specs=rows(3 * d), out_shape=jax.ShapeDtypeStruct((t, 3 * d), BF),
        compiler_params=_params(40, "arbitrary"), cost_estimate=_cost(6 * t * d * d, 8 * t * d + 6 * d * d),
    )(h, packed, packed, packed, cos, sin)


def _qkv_back_kernel(dq_ref, dk_ref, dv_ref, h_ref, cos_ref, sin_ref, *rest, first):
    if first:
        dw_ref, sum_s = rest
    else:
        wq_ref, wk_ref, wv_ref, up_ref, dw_ref, dh_ref, sum_s = rest
    i, d = pl.program_id(0), h_ref.shape[1]

    @pl.when(i == 0)
    def _():
        sum_s[...] = jnp.zeros_like(sum_s)

    h = h_ref[...]
    at = _normed(h)[0].astype(BF).T
    cos, sin = cos_ref[...], sin_ref[...]

    def turned_back(ref):
        parts = []
        for s in _heads(d):
            one = ref[:, s].astype(F32)
            parts.append((one * cos - pltpu.roll(one, HEAD // 2, 1) * sin).astype(BF))
        return jnp.concatenate(parts, 1)

    grads = [turned_back(dq_ref), turned_back(dk_ref), dv_ref[...]]
    for n, g in enumerate(grads):
        sum_s[:, n * d : (n + 1) * d] += _dot(at, g, 1, 0)
    if not first:
        by_a = [_dot(g, w[...], 1, 1).astype(BF) for g, w in zip(grads, (wq_ref, wk_ref, wv_ref))]
        by_a = (by_a[2] + by_a[1]) + by_a[0]
        dh_ref[...] = up_ref[...] + _norm_back(h, by_a)

    @pl.when(i == pl.num_programs(0) - 1)
    def _():
        dw_ref[...] = sum_s[...].astype(BF)


def qkv_backward(dq, dk, dv, h, cos, sin, packed=None, at=0, above=None, tile=512):
    t, d = h.shape
    rows = lambda n: pl.BlockSpec((tile, n), lambda i: (i, 0))
    weight = lambda j: pl.BlockSpec((d, d), lambda i: (0, j))
    first = packed is None
    specs, args = [rows(d)] * 4 + [rows(HEAD)] * 2, [dq, dk, dv, h, cos, sin]
    outs, shapes = [pl.BlockSpec((d, 3 * d), lambda i: (0, 0))], [jax.ShapeDtypeStruct((d, 3 * d), BF)]
    if not first:
        specs += [weight(at), weight(at + 1), weight(at + 2), rows(d)]
        args += [packed, packed, packed, above]
        outs += [rows(d)]
        shapes += [jax.ShapeDtypeStruct((t, d), BF)]
    return pl.pallas_call(
        functools.partial(_qkv_back_kernel, first=first), grid=(t // tile,), name="qkv_backward",
        in_specs=specs, out_specs=outs, out_shape=shapes, scratch_shapes=[pltpu.VMEM((d, 3 * d), F32)],
        compiler_params=_params(48, "arbitrary"), cost_estimate=_cost((6 if first else 12) * t * d * d, 12 * t * d + 12 * d * d),
    )(*args)


def _attend_kernel(q_ref, k_ref, v_ref, o_ref, lse_ref, top_s, mix_s, *, cut):
    iq, bq = pl.program_id(0), q_ref.shape[0]
    heads = _heads(q_ref.shape[1])
    scale = HEAD**-0.5
    e = scale * LOG2E
    for i in range(len(heads)):
        top_s[i : i + 1, :] = jnp.full((1, bq), NEG, F32)
        mix_s[i] = jnp.zeros(mix_s.shape[1:], F32)

    def block(start, bk, at, masked):
        here = pl.ds(start, bk)
        ones = jnp.ones((8, bk), BF)
        scores = [_dot(k_ref[here, s], q_ref[at:, s], 1, 1) for s in heads]
        if masked:
            shape = scores[0].shape
            ok = lax.broadcasted_iota(jnp.int32, shape, 1) >= lax.broadcasted_iota(jnp.int32, shape, 0)
        weights, keeps = [], []
        for i, s in enumerate(scores):
            if masked:
                s = jnp.where(ok, s, HIDDEN)
            old = top_s[i : i + 1, at:]
            top = jnp.maximum(old, s.max(axis=0, keepdims=True))
            top_s[i : i + 1, at:] = top
            weights.append(jnp.exp2((s - top) * e).astype(BF))
            keeps.append(jnp.exp2((old - top) * e))
        for i, (p, keep) in enumerate(zip(weights, keeps)):
            values = jnp.concatenate([v_ref[here, heads[i]].T, ones], axis=0)
            mix_s[i, :, at:] = mix_s[i, :, at:] * keep + _dot(values, p, 1, 0)

    lax.fori_loop(0, iq, lambda j, _: block(pl.multiple_of(j * bq, bq), bq, 0, False), None)
    for at in range(0, bq, cut):
        block(pl.multiple_of(iq * bq + at, cut), cut, at, True)
    for i, s in enumerate(heads):
        total = mix_s[i, HEAD : HEAD + 1, :]
        o_ref[:, s] = (mix_s[i, :HEAD, :] * (1 / total)).T.astype(BF)
        lse_ref[i : i + 1, :] = top_s[i : i + 1, :] * scale + jnp.log(total)


def attend(qkv, bq=512, cut=256):
    t, d = qkv.shape[0], qkv.shape[1] // 3
    n = d // HEAD
    return pl.pallas_call(
        functools.partial(_attend_kernel, cut=cut), grid=(t // bq,), name="attend",
        in_specs=[pl.BlockSpec((bq, d), lambda i: (i, 0)), pl.BlockSpec((t, d), lambda i: (0, 1)), pl.BlockSpec((t, d), lambda i: (0, 2))],
        out_specs=[pl.BlockSpec((bq, d), lambda i: (i, 0)), pl.BlockSpec((n, bq), lambda i: (0, i))],
        out_shape=[jax.ShapeDtypeStruct((t, d), BF), jax.ShapeDtypeStruct((n, t), F32)],
        scratch_shapes=[pltpu.VMEM((n, bq), F32), pltpu.VMEM((n, HEAD + 8, bq), F32)],
        compiler_params=_params(56, "arbitrary"), cost_estimate=_cost(4 * t * t * d, 8 * t * d),
    )(qkv, qkv, qkv)


def _attend_back_kernel(q_ref, k_ref, v_ref, o_ref, up_ref, wo_ref, lse_ref, dq_ref, dk_ref, dv_ref, dwo_ref,
                        dq_s, dk_s, dv_s, do_s, dwo_s, *, cut):
    iq, bq = pl.program_id(0), q_ref.shape[0]
    heads = _heads(q_ref.shape[1])
    scale = HEAD**-0.5
    e = scale * LOG2E

    @pl.when(iq == 0)
    def _():
        dk_s[...] = jnp.zeros_like(dk_s)
        dv_s[...] = jnp.zeros_like(dv_s)
        dwo_s[...] = jnp.zeros_like(dwo_s)

    dq_s[...] = jnp.zeros_like(dq_s)
    up = up_ref[...]
    do_s[...] = _dot(up, wo_ref[...], 1, 1).astype(BF)
    dwo_s[...] += _dot(o_ref[...].T, up, 1, 0)
    deltas = [(do_s[:, s].astype(F32) * o_ref[:, s].astype(F32)).T.sum(axis=0, keepdims=True) for s in heads]
    lses = [lse_ref[i : i + 1, :] * LOG2E for i in range(len(heads))]

    def block(start, bk, at, masked):
        here = pl.ds(start, bk)
        scores = [_dot(k_ref[here, s], q_ref[at:, s], 1, 1) for s in heads]
        dps = [_dot(v_ref[here, s], do_s[at:, s], 1, 1) for s in heads]
        if masked:
            shape = scores[0].shape
            ok = lax.broadcasted_iota(jnp.int32, shape, 1) >= lax.broadcasted_iota(jnp.int32, shape, 0)
        for i, s in enumerate(heads):
            p = jnp.exp2(scores[i] * e - lses[i][:, at:])
            if masked:
                p = jnp.where(ok, p, 0.0)
            ds = (p * (dps[i] - deltas[i][:, at:])).astype(BF)
            dv_s[here, s] += _dot(p.astype(BF), do_s[at:, s], 1, 0)
            dk_s[here, s] += _dot(ds, q_ref[at:, s], 1, 0)
            dq_s[i, :, at:] += _dot(k_ref[here, s].T, ds, 1, 0)

    lax.fori_loop(0, iq, lambda j, _: block(pl.multiple_of(j * bq, bq), bq, 0, False), None)
    for at in range(0, bq, cut):
        block(pl.multiple_of(iq * bq + at, cut), cut, at, True)
    for i, s in enumerate(heads):
        dq_ref[:, s] = (dq_s[i] * scale).T.astype(BF)

    @pl.when(iq == pl.num_programs(0) - 1)
    def _():
        dk_ref[...] = (dk_s[...] * scale).astype(BF)
        dv_ref[...] = dv_s[...].astype(BF)
        dwo_ref[...] = dwo_s[...].astype(BF)


def attend_backward(qkv, o, lse, above, packed, at, bq=512, cut=256):
    t, d = o.shape
    n = d // HEAD
    tile, whole = pl.BlockSpec((bq, d), lambda i: (i, 0)), lambda j: pl.BlockSpec((t, d), lambda i: (0, j))
    return pl.pallas_call(
        functools.partial(_attend_back_kernel, cut=cut), grid=(t // bq,), name="attend_backward",
        in_specs=[tile, whole(1), whole(2), tile, tile, pl.BlockSpec((d, d), lambda i: (0, at)), pl.BlockSpec((n, bq), lambda i: (0, i))],
        out_specs=[tile, whole(0), whole(0), pl.BlockSpec((d, d), lambda i: (0, 0))],
        out_shape=[jax.ShapeDtypeStruct((t, d), BF)] * 3 + [jax.ShapeDtypeStruct((d, d), BF)],
        scratch_shapes=[pltpu.VMEM((n, HEAD, bq), F32), pltpu.VMEM((t, d), F32), pltpu.VMEM((t, d), F32), pltpu.VMEM((bq, d), BF),
                        pltpu.VMEM((d, d), F32)],
        compiler_params=_params(60, "arbitrary"), cost_estimate=_cost(10 * t * t * d // 2 + 4 * t * d * d, 20 * t * d),
    )(qkv, qkv, qkv, o, above, packed, lse)


def _unpacked_down(ref, wide_s, out_s):
    d = out_s.shape[1]
    runs = ref.shape[1] // d
    for j in range(runs):
        piece = ref[:, j * d : (j + 1) * d].astype(F32)
        for e in range(ref.shape[0] // 40):
            wide_s[(e * runs + j) * 40 : (e * runs + j + 1) * 40, :] = piece[e * 40 : (e + 1) * 40]
    out_s[...] = wide_s[...].astype(BF)


def _ffn_kernel(o_ref, h_ref, wo_ref, gate_w, up_w, down_w, h2_ref, gate_ref, up_ref, y_ref, b_s, h2_s, y_s, down_s, wide_s):
    c, t, tile = pl.program_id(0), pl.program_id(1), h_ref.shape[0]
    here = pl.ds(pl.multiple_of(t * tile, tile), tile)

    @pl.when(c == 0)
    def _():
        h2 = h_ref[...] + _dot(o_ref[...], wo_ref[...], 1, 0).astype(BF)
        h2_ref[...] = h2
        h2_s[here, :] = h2
        b_s[here, :] = _normed(h2)[0].astype(BF)
        y_s[here, :] = jnp.zeros((tile, y_s.shape[1]), F32)

    @pl.when(t == 0)
    def _():
        _unpacked_down(down_w, wide_s, down_s)

    b = b_s[here, :]
    gate, up = _dot(b, gate_w[...], 1, 0), _dot(b, up_w[...], 1, 0)
    gate_ref[...] = gate
    up_ref[...] = up
    hidden = (gate * jax.nn.sigmoid(gate) * up).astype(BF)
    y_s[here, :] += _dot(hidden, down_s[...], 1, 0)

    @pl.when(c == pl.num_programs(0) - 1)
    def _():
        y_ref[...] = h2_s[here, :] + y_s[here, :].astype(BF)


def ffn_forward(o, h, packed, wo_at, gate_at, tile=512):
    t, d = h.shape
    chunks = 4
    last = t // tile - 1
    early = pl.BlockSpec((tile, d), lambda c, i: (jnp.where(c == 0, i, last), 0))
    late = pl.BlockSpec((tile, d), lambda c, i: (jnp.where(c == chunks - 1, i, 0), 0))
    inner = pl.BlockSpec((tile, d), lambda c, i: (i, c))
    return pl.pallas_call(
        _ffn_kernel, grid=(chunks, t // tile), name="ffn_forward",
        in_specs=[early, early, pl.BlockSpec((d, d), lambda c, i: (0, wo_at)), pl.BlockSpec((d, d), lambda c, i: (0, gate_at + c)),
                  pl.BlockSpec((d, d), lambda c, i: (0, gate_at + 4 + c)), pl.BlockSpec((d // 4, 4 * d), lambda c, i: (c, gate_at // 4 + 2))],
        out_specs=[early, inner, inner, late],
        out_shape=[jax.ShapeDtypeStruct((t, d), BF), jax.ShapeDtypeStruct((t, 4 * d), F32), jax.ShapeDtypeStruct((t, 4 * d), F32),
                   jax.ShapeDtypeStruct((t, d), BF)],
        scratch_shapes=[pltpu.VMEM((t, d), BF), pltpu.VMEM((t, d), BF), pltpu.VMEM((t, d), F32), pltpu.VMEM((d, d), BF), pltpu.VMEM((d, d), F32)],
        compiler_params=_params(60, "arbitrary", "arbitrary"), cost_estimate=_cost(2 * t * d * d * 13, 40 * t * d),
    )(o, h, packed, packed, packed, packed)


def _ffn_back_kernel(*refs, kept):
    if kept:
        h2_ref, gate_ref, up_ref, dy_ref, gate_w, up_w, down_w, *refs = refs
    else:
        o_ref, h_ref, wo_ref, dy_ref, gate_w, up_w, down_w, *refs = refs
    dh_ref, dw_ref, *refs = refs
    h2_s, b_s, bt_s, dyt_s, by_gate_s, by_up_s, dgate_s, dup_s, ddown_s, down_s, wide_s, stage_s, sems = refs
    c, t, tile, d = pl.program_id(0), pl.program_id(1), dy_ref.shape[0], dy_ref.shape[1]
    chunks, tiles = pl.num_programs(0), pl.num_programs(1)
    here = pl.ds(pl.multiple_of(t * tile, tile), tile)
    dy = dy_ref[...]

    def copies(chunk):
        whole = 4 * d
        col = lambda first: pl.ds(pl.multiple_of(first + chunk * d, d), d)
        out = [pltpu.make_async_copy(stage_s.at[n], dw_ref.at[:, col(n * whole)], sems.at[n]) for n in range(2)]
        rows = pl.ds(pl.multiple_of(chunk * (d // 4), d // 4), d // 4)
        for j in range(4):
            cols = pl.ds(2 * whole + j * d, d)
            out.append(pltpu.make_async_copy(stage_s.at[2, pl.ds(j * (d // 4), d // 4)], dw_ref.at[rows, cols], sems.at[2 + j]))
        return out

    @pl.when(c == 0)
    def _():
        if kept:
            h2 = h2_ref[...]
        else:
            h2 = h_ref[...] + _dot(o_ref[...], wo_ref[...], 1, 0).astype(BF)
        h2_s[here, :] = h2
        b = _normed(h2)[0].astype(BF)
        b_s[here, :] = b
        bt_s[:, here] = b.T
        dyt_s[:, here] = dy.T
        by_gate_s[here, :] = jnp.zeros((tile, d), F32)
        by_up_s[here, :] = jnp.zeros((tile, d), F32)

    @pl.when(t == 0)
    def _():
        _unpacked_down(down_w, wide_s, down_s)
        dgate_s[...] = jnp.zeros_like(dgate_s)
        dup_s[...] = jnp.zeros_like(dup_s)
        ddown_s[...] = jnp.zeros_like(ddown_s)

    if kept:
        gate, up = gate_ref[...], up_ref[...]
    else:
        b = b_s[here, :]
        gate, up = _dot(b, gate_w[...], 1, 0), _dot(b, up_w[...], 1, 0)
    by_hidden = _dot(dy, down_s[...], 1, 1).astype(BF).astype(F32)
    sig = jax.nn.sigmoid(gate)
    silu = gate * sig
    by_up = (by_hidden * silu).astype(BF)
    by_gate = (by_hidden * up * (sig * (1 + gate * (1 - sig)))).astype(BF)
    hidden = (silu * up).astype(BF)
    bt = bt_s[:, here]
    dgate_s[...] += _dot(bt, by_gate, 1, 0)
    dup_s[...] += _dot(bt, by_up, 1, 0)
    ddown_s[...] += _dot(dyt_s[:, here], hidden, 1, 0)
    by_gate_s[here, :] += _dot(by_gate, gate_w[...], 1, 1)
    by_up_s[here, :] += _dot(by_up, up_w[...], 1, 1)

    @pl.when(t == tiles - 1)
    def _():
        @pl.when(c > 0)
        def _():
            for one in copies(c - 1):
                one.wait()

        stage_s[0] = dgate_s[...].astype(BF)
        stage_s[1] = dup_s[...].astype(BF)
        wide_s[...] = ddown_s[...].T
        for j in range(4):
            for e in range(4):
                dgate_s[j * (d // 4) + e * 40 : j * (d // 4) + (e + 1) * 40, :] = wide_s[(e * 4 + j) * 40 : (e * 4 + j + 1) * 40, :]
        stage_s[2] = dgate_s[...].astype(BF)
        for one in copies(c):
            one.start()

        @pl.when(c == chunks - 1)
        def _():
            for one in copies(c):
                one.wait()

    @pl.when(c == chunks - 1)
    def _():
        by_b = by_up_s[here, :].astype(BF) + by_gate_s[here, :].astype(BF)
        dh_ref[...] = dy + _norm_back(h2_s[here, :], by_b)


def ffn_backward(dy, packed, gate_at, kept=None, fresh=None, wo_at=0, tile=512):
    t, d = dy.shape
    chunks = 4
    last = t // tile - 1
    early = pl.BlockSpec((tile, d), lambda c, i: (jnp.where(c == 0, i, last), 0))
    late = pl.BlockSpec((tile, d), lambda c, i: (jnp.where(c == chunks - 1, i, 0), 0))
    inner = pl.BlockSpec((tile, d), lambda c, i: (i, c))
    if kept is not None:
        specs, args = [early, inner, inner], list(kept)
    else:
        specs, args = [early, early, pl.BlockSpec((d, d), lambda c, i: (0, wo_at))], [*fresh, packed]
    specs += [pl.BlockSpec((tile, d), lambda c, i: (i, 0)), pl.BlockSpec((d, d), lambda c, i: (0, gate_at + c)),
              pl.BlockSpec((d, d), lambda c, i: (0, gate_at + 4 + c)), pl.BlockSpec((d // 4, 4 * d), lambda c, i: (c, gate_at // 4 + 2))]
    return pl.pallas_call(
        functools.partial(_ffn_back_kernel, kept=kept is not None), grid=(chunks, t // tile), name="ffn_backward",
        in_specs=specs, out_specs=[late, pl.BlockSpec(memory_space=pl.ANY)],
        out_shape=[jax.ShapeDtypeStruct((t, d), BF), jax.ShapeDtypeStruct((d, 12 * d), BF)],
        scratch_shapes=[pltpu.VMEM((t, d), BF), pltpu.VMEM((t, d), BF), pltpu.VMEM((d, t), BF), pltpu.VMEM((d, t), BF), pltpu.VMEM((t, d), F32),
                        pltpu.VMEM((t, d), F32), pltpu.VMEM((d, d), F32), pltpu.VMEM((d, d), F32), pltpu.VMEM((d, d), F32),
                        pltpu.VMEM((d, d), BF), pltpu.VMEM((d, d), F32), pltpu.VMEM((3, d, d), BF), pltpu.SemaphoreType.DMA((6,))],
        compiler_params=_params(62, "arbitrary", "arbitrary"), cost_estimate=_cost(2 * t * d * d * (24 if kept is not None else 33), 60 * t * d),
    )(*args, dy, packed, packed, packed)


def adamw(w, m, v, g):
    m = 0.9 * m + 0.1 * g
    v = 0.95 * v + 0.05 * g * g
    step = m * lax.rsqrt(v + 1e-8) + 0.1 * w
    return (w - 0.02 * step).astype(BF), m, v


def sideways(w):
    rows = w.shape[0] // 4
    return w.reshape(4, rows, -1).transpose(1, 0, 2).reshape(rows, -1)


def upright(w):
    rows, d = w.shape[0], w.shape[1] // 4
    return w.reshape(rows, 4, d).transpose(1, 0, 2).reshape(4 * rows, d)


def solution(mesh):
    def step(x, dy, *arrays):
        weights, m, v = (arrays[i : i + 7] for i in (0, 7, 14))
        wq, wk, wv, wo, w_gate, w_up, w_down = weights
        t, d = x.shape[1], x.shape[2]
        half = HEAD // 2
        angle = jnp.arange(t, dtype=F32)[:, None] * THETA ** (-jnp.arange(half, dtype=F32) / half)
        cos, sin = jnp.cos(angle), jnp.sin(angle)
        cos, sin = jnp.concatenate([cos, cos], 1), jnp.concatenate([-sin, sin], 1)

        def gathered(parts):
            return lax.all_gather(jnp.concatenate(parts, axis=1), "dp", axis=0, tiled=True)

        head = gathered([wq[0], wk[0], wv[0]])
        rest = gathered([w_gate[0], w_up[0], sideways(w_down[0]), w_gate[1], w_up[1], sideways(w_down[1]), wq[1], wk[1], wv[1], wo[1], wo[0]])
        GATE, QKV, WO = (0, 12), (0, 24), (28, 27)

        h0 = x[0]
        qkv0 = qkv_forward(h0, head, 0, cos, sin)
        o0, lse0 = attend(qkv0)
        mid0, gate0, up0, h1 = ffn_forward(o0, h0, rest, WO[0], GATE[0])
        qkv1 = qkv_forward(h1, rest, QKV[1], cos, sin)
        o1, lse1 = attend(qkv1)
        by_mid1, ffn1 = ffn_backward(dy[0], rest, GATE[1], fresh=(o1, h1), wo_at=WO[1])

        def scattered(g):
            return lax.psum_scatter(g, "dp", scatter_dimension=0, tiled=True)

        got_ffn1 = scattered(ffn1)
        dq1, dk1, dv1, dwo1 = attend_backward(qkv1, o1, lse1, by_mid1, rest, WO[1])
        dqkv1, by_h1 = qkv_backward(dq1, dk1, dv1, h1, cos, sin, rest, QKV[1], by_mid1)
        got_attn1 = scattered(jnp.concatenate([dqkv1, dwo1], 1))
        by_mid0, ffn0 = ffn_backward(by_h1, rest, GATE[0], kept=(mid0, gate0, up0))
        got_ffn0 = scattered(ffn0)
        dq0, dk0, dv0, dwo0 = attend_backward(qkv0, o0, lse0, by_mid0, rest, WO[0])
        (dqkv0,) = qkv_backward(dq0, dk0, dv0, h0, cos, sin)
        got_attn0 = scattered(jnp.concatenate([dqkv0, dwo0], 1))

        got = [[got_attn0, got_ffn0], [got_attn1, got_ffn1]]
        squares = sum(jnp.sum(jnp.square(g.astype(F32))) for one in got for g in one)
        squares = lax.psum(squares, "dp")
        count = lax.psum(1, "dp") * sum(w.size for w in weights)
        factor = jnp.minimum(1.0, 0.5 * lax.rsqrt(squares / count + 1e-30))

        def gradient(number, name):
            attn, ffn = got[number]
            if name < 4:
                return attn[:, name * d : (name + 1) * d]
            part = ffn[:, (name - 4) * 4 * d : (name - 3) * 4 * d]
            return part if name < 6 else upright(part)

        new = []
        for name in range(7):
            g = jnp.stack([gradient(0, name), gradient(1, name)]).astype(F32) * factor
            new.append(adamw(weights[name].astype(F32), m[name], v[name], g))
        return tuple(one[which] for which in range(3) for one in new)

    states, cut = P(("rep", "dp"), None, None), P(None, "dp", None)
    return jax.shard_map(
        step,
        mesh=mesh,
        in_specs=(states, states) + (cut,) * 21,
        out_specs=(P("rep", "dp", None),) * 21,
        check_vma=False,
    )
```

```python
import functools

import jax
import jax.numpy as jnp
from jax import lax
from jax.experimental import pallas as pl
from jax.experimental.pallas import tpu as pltpu
from jax.sharding import PartitionSpec as P


NEG = -1e30
HIDDEN = 2 * NEG
LOG2E = 1.4426950408889634
HEAD = 128
THETA = 10000
BF, F32 = jnp.bfloat16, jnp.float32
MiB = 2**20
PARTS = 1


def _dot(a, b, ca, cb):
    return lax.dot_general(a, b, (((ca,), (cb,)), ((), ())), preferred_element_type=F32)


def _mm(a, b):
    return _dot(a, b, 1, 0)


def _mt(a, b):
    return _dot(a, b, 1, 1)


def _params(limit, *axes):
    return pltpu.CompilerParams(dimension_semantics=axes, vmem_limit_bytes=limit * MiB)


def _rows(tile, n):
    return pl.BlockSpec((tile, n), lambda i: (i, 0))


def _block(shape, *at):
    return pl.BlockSpec(shape, lambda *_: at)


def _cost(flops, size):
    return pl.CostEstimate(flops=int(flops), transcendentals=0, bytes_accessed=int(size))


def _normed(h):
    wide = h.astype(F32)
    scale = lax.rsqrt(jnp.mean(wide * wide, -1, keepdims=True) + 1e-6)
    return wide * scale, scale


def _norm_back(h, by_n):
    wide, by_n = h.astype(F32), by_n.astype(F32)
    scale = lax.rsqrt(jnp.mean(wide * wide, -1, keepdims=True) + 1e-6)
    inner = jnp.mean(by_n * wide, -1, keepdims=True)
    return (by_n * scale - wide * (scale * scale * scale * inner)).astype(BF)


def _heads(width):
    return [slice(i, i + HEAD) for i in range(0, width, HEAD)]


def _qkv_kernel(h_ref, wq_ref, wk_ref, wv_ref, cos_ref, sin_ref, out_ref):
    d = h_ref.shape[1]
    a = _normed(h_ref[...])[0].astype(BF)
    cos, sin = cos_ref[...], sin_ref[...]
    for n, w_ref in enumerate((wq_ref, wk_ref)):
        t = _mm(a, w_ref[...]).astype(BF).astype(F32)
        for s in _heads(d):
            one = t[:, s]
            out_ref[:, n * d + s.start : n * d + s.stop] = (one * cos + pltpu.roll(one, HEAD // 2, 1) * sin).astype(BF)
    out_ref[:, 2 * d :] = _mm(a, wv_ref[...]).astype(BF)


def qkv_forward(h, packed, at, cos, sin, tile=512):
    t, d = h.shape
    rows, weight = functools.partial(_rows, tile), functools.partial(_block, (d, d), 0)
    return pl.pallas_call(
        _qkv_kernel, grid=(t // tile,), name="qkv_forward",
        in_specs=[rows(d), weight(at), weight(at + 1), weight(at + 2), rows(HEAD), rows(HEAD)],
        out_specs=rows(3 * d), out_shape=jax.ShapeDtypeStruct((t, 3 * d), BF),
        compiler_params=_params(40, "arbitrary"), cost_estimate=_cost(6 * t * d * d, 8 * t * d + 6 * d * d),
    )(h, packed, packed, packed, cos, sin)


def _qkv_back_kernel(dq_ref, dk_ref, dv_ref, h_ref, cos_ref, sin_ref, *rest, first):
    if first:
        dw_ref, sum_s = rest
    else:
        wq_ref, wk_ref, wv_ref, up_ref, dw_ref, dh_ref, sum_s = rest
    i, d = pl.program_id(0), h_ref.shape[1]

    @pl.when(i == 0)
    def _():
        sum_s[...] = jnp.zeros_like(sum_s)

    h = h_ref[...]
    at = _normed(h)[0].astype(BF).T
    cos, sin = cos_ref[...], sin_ref[...]

    def turned_back(ref):
        parts = []
        for s in _heads(d):
            one = ref[:, s].astype(F32)
            parts.append((one * cos - pltpu.roll(one, HEAD // 2, 1) * sin).astype(BF))
        return jnp.concatenate(parts, 1)

    grads = [turned_back(dq_ref), turned_back(dk_ref), dv_ref[...]]
    for n, g in enumerate(grads):
        sum_s[:, n * d : (n + 1) * d] += _mm(at, g)
    if not first:
        by_a = [_mt(g, w[...]).astype(BF) for g, w in zip(grads, (wq_ref, wk_ref, wv_ref))]
        by_a = (by_a[2] + by_a[1]) + by_a[0]
        dh_ref[...] = up_ref[...] + _norm_back(h, by_a)

    @pl.when(i == pl.num_programs(0) - 1)
    def _():
        dw_ref[...] = sum_s[...].astype(BF)


def qkv_backward(dq, dk, dv, h, cos, sin, packed=None, at=0, above=None, tile=512):
    t, d = h.shape
    rows, weight = functools.partial(_rows, tile), functools.partial(_block, (d, d), 0)
    first = packed is None
    specs, args = [rows(d)] * 4 + [rows(HEAD)] * 2, [dq, dk, dv, h, cos, sin]
    outs, shapes = [_block((d, 3 * d), 0, 0)], [jax.ShapeDtypeStruct((d, 3 * d), BF)]
    if not first:
        specs += [weight(at), weight(at + 1), weight(at + 2), rows(d)]
        args += [packed, packed, packed, above]
        outs += [rows(d)]
        shapes += [jax.ShapeDtypeStruct((t, d), BF)]
    return pl.pallas_call(
        functools.partial(_qkv_back_kernel, first=first), grid=(t // tile,), name="qkv_backward",
        in_specs=specs, out_specs=outs, out_shape=shapes, scratch_shapes=[pltpu.VMEM((d, 3 * d), F32)],
        compiler_params=_params(48, "arbitrary"), cost_estimate=_cost((6 if first else 12) * t * d * d, 12 * t * d + 12 * d * d),
    )(*args)


def _attend_kernel(q_ref, k_ref, v_ref, o_ref, lse_ref, top_s, mix_s, *, cut):
    iq, bq = pl.program_id(0), q_ref.shape[0]
    heads = _heads(q_ref.shape[1])
    scale = HEAD**-0.5
    e = scale * LOG2E
    for i in range(len(heads)):
        top_s[i : i + 1, :] = jnp.full((1, bq), NEG, F32)
        mix_s[i] = jnp.zeros(mix_s.shape[1:], F32)

    def block(start, bk, at, masked):
        here = pl.ds(start, bk)
        ones = jnp.ones((8, bk), BF)
        scores = [_mt(k_ref[here, s], q_ref[at:, s]) for s in heads]
        if masked:
            shape = scores[0].shape
            ok = lax.broadcasted_iota(jnp.int32, shape, 1) >= lax.broadcasted_iota(jnp.int32, shape, 0)
        weights, keeps = [], []
        for i, s in enumerate(scores):
            if masked:
                s = jnp.where(ok, s, HIDDEN)
            old = top_s[i : i + 1, at:]
            top = jnp.maximum(old, s.max(axis=0, keepdims=True))
            top_s[i : i + 1, at:] = top
            weights.append(jnp.exp2((s - top) * e).astype(BF))
            keeps.append(jnp.exp2((old - top) * e))
        for i, (p, keep) in enumerate(zip(weights, keeps)):
            values = jnp.concatenate([v_ref[here, heads[i]].T, ones], axis=0)
            mix_s[i, :, at:] = mix_s[i, :, at:] * keep + _mm(values, p)

    lax.fori_loop(0, iq, lambda j, _: block(pl.multiple_of(j * bq, bq), bq, 0, False), None)
    for at in range(0, bq, cut):
        block(pl.multiple_of(iq * bq + at, cut), cut, at, True)
    for i, s in enumerate(heads):
        total = mix_s[i, HEAD : HEAD + 1, :]
        o_ref[:, s] = (mix_s[i, :HEAD, :] * (1 / total)).T.astype(BF)
        lse_ref[i : i + 1, :] = top_s[i : i + 1, :] * scale + jnp.log(total)


def attend(qkv, bq=512, cut=256):
    t, d = qkv.shape[0], qkv.shape[1] // 3
    n = d // HEAD
    return pl.pallas_call(
        functools.partial(_attend_kernel, cut=cut), grid=(t // bq,), name="attend",
        in_specs=[_rows(bq, d), _block((t, d), 0, 1), _block((t, d), 0, 2)],
        out_specs=[_rows(bq, d), pl.BlockSpec((n, bq), lambda i: (0, i))],
        out_shape=[jax.ShapeDtypeStruct((t, d), BF), jax.ShapeDtypeStruct((n, t), F32)],
        scratch_shapes=[pltpu.VMEM((n, bq), F32), pltpu.VMEM((n, HEAD + 8, bq), F32)],
        compiler_params=_params(56, "arbitrary"), cost_estimate=_cost(4 * t * t * d, 8 * t * d),
    )(qkv, qkv, qkv)


def _attend_back_kernel(q_ref, k_ref, v_ref, o_ref, up_ref, wo_ref, lse_ref, dq_ref, dk_ref, dv_ref, dwo_ref,
                        dq_s, dk_s, dv_s, do_s, dwo_s, *, cut):
    iq, bq = pl.program_id(0), q_ref.shape[0]
    heads = _heads(q_ref.shape[1])
    scale = HEAD**-0.5
    e = scale * LOG2E

    @pl.when(iq == 0)
    def _():
        dk_s[...] = jnp.zeros_like(dk_s)
        dv_s[...] = jnp.zeros_like(dv_s)
        dwo_s[...] = jnp.zeros_like(dwo_s)

    dq_s[...] = jnp.zeros_like(dq_s)
    up = up_ref[...]
    do_s[...] = _mt(up, wo_ref[...]).astype(BF)
    dwo_s[...] += _mm(o_ref[...].T, up)
    deltas = [(do_s[:, s].astype(F32) * o_ref[:, s].astype(F32)).T.sum(axis=0, keepdims=True) for s in heads]
    lses = [lse_ref[i : i + 1, :] * LOG2E for i in range(len(heads))]

    def block(start, bk, at, masked):
        here = pl.ds(start, bk)
        scores = [_mt(k_ref[here, s], q_ref[at:, s]) for s in heads]
        dps = [_mt(v_ref[here, s], do_s[at:, s]) for s in heads]
        if masked:
            shape = scores[0].shape
            ok = lax.broadcasted_iota(jnp.int32, shape, 1) >= lax.broadcasted_iota(jnp.int32, shape, 0)
        for i, s in enumerate(heads):
            p = jnp.exp2(scores[i] * e - lses[i][:, at:])
            if masked:
                p = jnp.where(ok, p, 0.0)
            ds = (p * (dps[i] - deltas[i][:, at:])).astype(BF)
            dv_s[here, s] += _mm(p.astype(BF), do_s[at:, s])
            dk_s[here, s] += _mm(ds, q_ref[at:, s])
            dq_s[i, :, at:] += _mm(k_ref[here, s].T, ds)

    lax.fori_loop(0, iq, lambda j, _: block(pl.multiple_of(j * bq, bq), bq, 0, False), None)
    for at in range(0, bq, cut):
        block(pl.multiple_of(iq * bq + at, cut), cut, at, True)
    for i, s in enumerate(heads):
        dq_ref[:, s] = (dq_s[i] * scale).T.astype(BF)

    @pl.when(iq == pl.num_programs(0) - 1)
    def _():
        dk_ref[...] = (dk_s[...] * scale).astype(BF)
        dv_ref[...] = dv_s[...].astype(BF)
        dwo_ref[...] = dwo_s[...].astype(BF)


def attend_backward(qkv, o, lse, above, packed, at, bq=512, cut=256):
    t, d = o.shape
    n = d // HEAD
    tile, whole = _rows(bq, d), functools.partial(_block, (t, d), 0)
    return pl.pallas_call(
        functools.partial(_attend_back_kernel, cut=cut), grid=(t // bq,), name="attend_backward",
        in_specs=[tile, whole(1), whole(2), tile, tile, _block((d, d), 0, at), pl.BlockSpec((n, bq), lambda i: (0, i))],
        out_specs=[tile, whole(0), whole(0), _block((d, d), 0, 0)],
        out_shape=[jax.ShapeDtypeStruct((t, d), BF)] * 3 + [jax.ShapeDtypeStruct((d, d), BF)],
        scratch_shapes=[pltpu.VMEM((n, HEAD, bq), F32), pltpu.VMEM((t, d), F32), pltpu.VMEM((t, d), F32), pltpu.VMEM((bq, d), BF),
                        pltpu.VMEM((d, d), F32)],
        compiler_params=_params(60, "arbitrary"), cost_estimate=_cost(10 * t * t * d // 2 + 4 * t * d * d, 20 * t * d),
    )(qkv, qkv, qkv, o, above, packed, lse)


def _unpacked_down(ref, wide_s, out_s):
    d = out_s.shape[1]
    runs = ref.shape[1] // d
    for j in range(runs):
        piece = ref[:, j * d : (j + 1) * d].astype(F32)
        for e in range(ref.shape[0] // 40):
            wide_s[(e * runs + j) * 40 : (e * runs + j + 1) * 40, :] = piece[e * 40 : (e + 1) * 40]
    out_s[...] = wide_s[...].astype(BF)


def _ffn_kernel(o_ref, h_ref, wo_ref, gate_w, up_w, down_w, h2_ref, gate_ref, up_ref, y_ref, b_s, h2_s, y_s, down_s, wide_s):
    c, t, tile = pl.program_id(0), pl.program_id(1), h_ref.shape[0]
    here = pl.ds(pl.multiple_of(t * tile, tile), tile)

    @pl.when(c == 0)
    def _():
        h2 = h_ref[...] + _mm(o_ref[...], wo_ref[...]).astype(BF)
        h2_ref[...] = h2
        h2_s[here, :] = h2
        b_s[here, :] = _normed(h2)[0].astype(BF)
        y_s[here, :] = jnp.zeros((tile, y_s.shape[1]), F32)

    @pl.when(t == 0)
    def _():
        _unpacked_down(down_w, wide_s, down_s)

    size = tile // PARTS
    for at in range(0, tile, size):
        rows = pl.ds(pl.multiple_of(t * tile + at, size), size)
        b = b_s[rows, :]
        gate, up = _mm(b, gate_w[...]), _mm(b, up_w[...])
        gate_ref[at : at + size, :] = gate
        up_ref[at : at + size, :] = up
        hidden = (gate * jax.nn.sigmoid(gate) * up).astype(BF)
        y_s[rows, :] += _mm(hidden, down_s[...])

    @pl.when(c == pl.num_programs(0) - 1)
    def _():
        y_ref[...] = h2_s[here, :] + y_s[here, :].astype(BF)


def ffn_forward(o, h, packed, wo_at, gate_at, tile=512):
    t, d = h.shape
    chunks = 4
    last = t // tile - 1
    early = pl.BlockSpec((tile, d), lambda c, i: (jnp.where(c == 0, i, last), 0))
    late = pl.BlockSpec((tile, d), lambda c, i: (jnp.where(c == chunks - 1, i, 0), 0))
    inner = pl.BlockSpec((tile, d), lambda c, i: (i, c))
    return pl.pallas_call(
        _ffn_kernel, grid=(chunks, t // tile), name="ffn_forward",
        in_specs=[early, early, _block((d, d), 0, wo_at), pl.BlockSpec((d, d), lambda c, i: (0, gate_at + c)),
                  pl.BlockSpec((d, d), lambda c, i: (0, gate_at + 4 + c)), pl.BlockSpec((d // 4, 4 * d), lambda c, i: (c, gate_at // 4 + 2))],
        out_specs=[early, inner, inner, late],
        out_shape=[jax.ShapeDtypeStruct((t, d), BF), jax.ShapeDtypeStruct((t, 4 * d), F32), jax.ShapeDtypeStruct((t, 4 * d), F32),
                   jax.ShapeDtypeStruct((t, d), BF)],
        scratch_shapes=[pltpu.VMEM((t, d), BF), pltpu.VMEM((t, d), BF), pltpu.VMEM((t, d), F32), pltpu.VMEM((d, d), BF), pltpu.VMEM((d, d), F32)],
        compiler_params=_params(62, "arbitrary", "arbitrary"), cost_estimate=_cost(2 * t * d * d * 13, 40 * t * d),
    )(o, h, packed, packed, packed, packed)


def _ffn_back_kernel(*refs, kept):
    if kept:
        h2_ref, gate_ref, up_ref, dy_ref, gate_w, up_w, down_w, *refs = refs
    else:
        o_ref, h_ref, wo_ref, dy_ref, gate_w, up_w, down_w, *refs = refs
    dh_ref, dw_ref, *refs = refs
    h2_s, b_s, bt_s, dyt_s, by_gate_s, by_up_s, dgate_s, dup_s, ddown_s, down_s, wide_s, stage_s, sems = refs
    c, t, tile, d = pl.program_id(0), pl.program_id(1), dy_ref.shape[0], dy_ref.shape[1]
    chunks, tiles = pl.num_programs(0), pl.num_programs(1)
    here = pl.ds(pl.multiple_of(t * tile, tile), tile)
    dy = dy_ref[...]

    def copies(chunk):
        whole = 4 * d
        col = lambda first: pl.ds(pl.multiple_of(first + chunk * d, d), d)
        out = [pltpu.make_async_copy(stage_s.at[n], dw_ref.at[:, col(n * whole)], sems.at[n]) for n in range(2)]
        rows = pl.ds(pl.multiple_of(chunk * (d // 4), d // 4), d // 4)
        for j in range(4):
            cols = pl.ds(2 * whole + j * d, d)
            out.append(pltpu.make_async_copy(stage_s.at[2, pl.ds(j * (d // 4), d // 4)], dw_ref.at[rows, cols], sems.at[2 + j]))
        return out

    @pl.when(c == 0)
    def _():
        if kept:
            h2 = h2_ref[...]
        else:
            h2 = h_ref[...] + _mm(o_ref[...], wo_ref[...]).astype(BF)
        h2_s[here, :] = h2
        b = _normed(h2)[0].astype(BF)
        b_s[here, :] = b
        bt_s[:, here] = b.T
        dyt_s[:, here] = dy.T
        by_gate_s[here, :] = jnp.zeros((tile, d), F32)
        by_up_s[here, :] = jnp.zeros((tile, d), F32)

    @pl.when(t == 0)
    def _():
        _unpacked_down(down_w, wide_s, down_s)
        dgate_s[...] = jnp.zeros_like(dgate_s)
        dup_s[...] = jnp.zeros_like(dup_s)
        ddown_s[...] = jnp.zeros_like(ddown_s)

    parts = []
    size = tile // PARTS
    for at in range(0, tile, size):
        part = slice(at, at + size)
        if kept:
            gate, up = gate_ref[part, :], up_ref[part, :]
        else:
            b = b_s[pl.ds(pl.multiple_of(t * tile + at, size), size), :]
            gate, up = _mm(b, gate_w[...]), _mm(b, up_w[...])
        by_hidden = _mt(dy_ref[part, :], down_s[...]).astype(BF).astype(F32)
        sig = jax.nn.sigmoid(gate)
        silu = gate * sig
        by_gate = by_hidden * up * (sig * (1 + gate * (1 - sig)))
        parts.append([one.astype(BF) for one in (by_gate, by_hidden * silu, silu * up)])
    by_gate, by_up, hidden = (jnp.concatenate(one, axis=0) for one in zip(*parts))
    bt = bt_s[:, here]
    dgate_s[...] += _mm(bt, by_gate)
    dup_s[...] += _mm(bt, by_up)
    ddown_s[...] += _mm(dyt_s[:, here], hidden)
    by_gate_s[here, :] += _mt(by_gate, gate_w[...])
    by_up_s[here, :] += _mt(by_up, up_w[...])

    @pl.when(t == tiles - 1)
    def _():
        @pl.when(c > 0)
        def _():
            for one in copies(c - 1):
                one.wait()

        stage_s[0] = dgate_s[...].astype(BF)
        stage_s[1] = dup_s[...].astype(BF)
        wide_s[...] = ddown_s[...].T
        for j in range(4):
            for e in range(4):
                dgate_s[j * (d // 4) + e * 40 : j * (d // 4) + (e + 1) * 40, :] = wide_s[(e * 4 + j) * 40 : (e * 4 + j + 1) * 40, :]
        stage_s[2] = dgate_s[...].astype(BF)
        for one in copies(c):
            one.start()

        @pl.when(c == chunks - 1)
        def _():
            for one in copies(c):
                one.wait()

    @pl.when(c == chunks - 1)
    def _():
        by_b = by_up_s[here, :].astype(BF) + by_gate_s[here, :].astype(BF)
        dh_ref[...] = dy + _norm_back(h2_s[here, :], by_b)


def ffn_backward(dy, packed, gate_at, kept=None, fresh=None, wo_at=0, tile=512):
    t, d = dy.shape
    chunks = 4
    last = t // tile - 1
    early = pl.BlockSpec((tile, d), lambda c, i: (jnp.where(c == 0, i, last), 0))
    late = pl.BlockSpec((tile, d), lambda c, i: (jnp.where(c == chunks - 1, i, 0), 0))
    inner = pl.BlockSpec((tile, d), lambda c, i: (i, c))
    if kept is not None:
        specs, args = [early, inner, inner], list(kept)
    else:
        specs, args = [early, early, _block((d, d), 0, wo_at)], [*fresh, packed]
    specs += [pl.BlockSpec((tile, d), lambda c, i: (i, 0)), pl.BlockSpec((d, d), lambda c, i: (0, gate_at + c)),
              pl.BlockSpec((d, d), lambda c, i: (0, gate_at + 4 + c)), pl.BlockSpec((d // 4, 4 * d), lambda c, i: (c, gate_at // 4 + 2))]
    return pl.pallas_call(
        functools.partial(_ffn_back_kernel, kept=kept is not None), grid=(chunks, t // tile), name="ffn_backward",
        in_specs=specs, out_specs=[late, pl.BlockSpec(memory_space=pl.ANY)],
        out_shape=[jax.ShapeDtypeStruct((t, d), BF), jax.ShapeDtypeStruct((d, 12 * d), BF)],
        scratch_shapes=[pltpu.VMEM((t, d), BF), pltpu.VMEM((t, d), BF), pltpu.VMEM((d, t), BF), pltpu.VMEM((d, t), BF), pltpu.VMEM((t, d), F32),
                        pltpu.VMEM((t, d), F32), pltpu.VMEM((d, d), F32), pltpu.VMEM((d, d), F32), pltpu.VMEM((d, d), F32),
                        pltpu.VMEM((d, d), BF), pltpu.VMEM((d, d), F32), pltpu.VMEM((3, d, d), BF), pltpu.SemaphoreType.DMA((6,))],
        compiler_params=_params(62, "arbitrary", "arbitrary"), cost_estimate=_cost(2 * t * d * d * (24 if kept is not None else 33), 60 * t * d),
    )(*args, dy, packed, packed, packed)


MESH = pl.DeviceIdType.MESH


def _place():
    me = lax.axis_index("dp")
    return me // 8, (me // 2) % 4, me % 2


def _at(y, z, c):
    return (y * 4 + z) * 2 + c


def _remote(src, dst, send, recv, to):
    return pltpu.make_async_remote_copy(src_ref=src, dst_ref=dst, send_sem=send, recv_sem=recv, device_id={"dp": to}, device_id_type=MESH)


def _greet(peers):
    barrier = pltpu.get_barrier_semaphore()
    for peer in peers:
        pl.semaphore_signal(barrier, inc=1, device_id={"dp": peer}, device_id_type=MESH)
    pl.semaphore_wait(barrier, len(peers))


def _gather_kernel(x_ref, out_ref, send, recv, own):
    y, z, c = _place()
    me = _at(y, z, c)
    line = [(z + k) % 4 for k in (1, 2, 3)]
    over, twin = _at(1 - y, z, c), _at(y, z, 1 - c)
    _greet([_at(y, k, c) for k in line] + [over, twin])
    mine = pltpu.make_async_copy(x_ref, out_ref.at[me], own)
    mine.start()
    sent = [_remote(x_ref, out_ref.at[me], send.at[n], recv.at[me], _at(y, k, c)) for n, k in enumerate(line)]
    sent += [_remote(x_ref, out_ref.at[me], send.at[3], recv.at[me], over), _remote(x_ref, out_ref.at[me], send.at[4], recv.at[me], twin)]
    for one in sent:
        one.start()

    def arrived(slot):
        _remote(x_ref, out_ref.at[slot], send.at[0], recv.at[slot], twin).wait_recv()

    def passed(slot, n, to):
        one = _remote(out_ref.at[slot], out_ref.at[slot], send.at[n], recv.at[slot], to)
        one.start()
        sent.append(one)

    for n, k in enumerate(line):
        slot = _at(y, k, c)
        arrived(slot)
        passed(slot, 5 + n, over)
        passed(slot, 8 + n, twin)
    for n, k in enumerate([z] + line):
        slot = _at(1 - y, k, c)
        arrived(slot)
        passed(slot, 11 + n, twin)
    for k in range(4):
        for row in range(2):
            arrived(_at(row, k, 1 - c))
    for one in sent:
        one.wait_send()
    mine.wait()


def gather_rows(x):
    rows, n = x.shape
    out = pl.pallas_call(
        _gather_kernel, name="gather_rows",
        in_specs=[pl.BlockSpec(memory_space=pltpu.VMEM)], out_specs=pl.BlockSpec(memory_space=pl.ANY),
        out_shape=jax.ShapeDtypeStruct((16, rows, n), x.dtype),
        scratch_shapes=[pltpu.SemaphoreType.DMA((15,)), pltpu.SemaphoreType.DMA((16,)), pltpu.SemaphoreType.DMA],
        compiler_params=pltpu.CompilerParams(collective_id=1, has_side_effects=True),
        cost_estimate=_cost(MiB, x.size),
    )(x)
    return out.reshape(16 * rows, n)


def _sum_kernel(*refs, cols):
    n = len(cols)
    ins, (out_ref, own, from_twin, ours, from_over, row, from_line, final), sems = refs[:n], refs[n : n + 8], refs[n + 8 :]
    load, twin_send, twin_recv, over_send, over_recv, line_send, line_recv, store = sems
    y, z, c = _place()
    line = [(z + k) % 4 for k in (1, 2, 3)]
    over, twin = _at(1 - y, z, c), _at(y, z, 1 - c)
    _greet([_at(y, k, c) for k in line] + [over, twin])
    d = own.shape[3]
    places = [(ref, at) for ref, width in zip(ins, cols) for at in range(0, width, d)]
    pieces = len(places)
    for p, (ref, at) in enumerate(places):
        _remote(ref.at[:, 1 - c, :, pl.ds(at, d)], from_twin.at[p], twin_send.at[p], twin_recv.at[p], twin).start()
        pltpu.make_async_copy(ref.at[:, c, :, pl.ds(at, d)], own.at[p], load.at[p]).start()

    def to_twin(p):
        return _remote(own.at[p], from_twin.at[p], twin_send.at[p], twin_recv.at[p], twin)

    def to_over(p):
        return _remote(ours.at[p, 1 - y], from_over.at[p], over_send.at[p], over_recv.at[p], over)

    def to_line(p, n, k):
        return _remote(row.at[p, k], from_line.at[p, z], line_send.at[p, n], line_recv.at[p, z], _at(y, k, c))

    def chip(p, _):
        pltpu.make_async_copy(own.at[p], own.at[p], load.at[p]).wait()
        to_twin(p).wait_recv()
        for yy in range(2):
            a, b = own[p, yy * 4 : yy * 4 + 4], from_twin[p, yy * 4 : yy * 4 + 4]
            ours[p, yy] = (a.astype(F32) + b.astype(F32)).astype(BF)
        to_over(p).start()

    def across(p, _):
        to_over(p).wait_recv()
        row[p] = (ours[p, y].astype(F32) + from_over[p].astype(F32)).astype(BF)
        for n, k in enumerate(line):
            to_line(p, n, k).start()

    def along(p, _):
        total = row[p, z].astype(F32)
        for k in line:
            _remote(row.at[p, k], from_line.at[p, k], line_send.at[p, 0], line_recv.at[p, k], twin).wait_recv()
            total = total + from_line[p, k].astype(F32)
        final[p] = total.astype(BF)

    def drained(p, _):
        to_twin(p).wait_send()
        to_over(p).wait_send()
        for n, k in enumerate(line):
            to_line(p, n, k).wait_send()

    for part in (chip, across, along, drained):
        lax.fori_loop(0, pieces, part, None)
    for p in range(pieces):
        pltpu.make_async_copy(final.at[p], out_ref.at[:, pl.ds(p * d, d)], store.at[p]).start()
    for p in range(pieces):
        pltpu.make_async_copy(final.at[p], out_ref.at[:, pl.ds(p * d, d)], store.at[p]).wait()


def scatter_sums(grads):
    d, cols = grads[0].shape[0], tuple(g.shape[1] for g in grads)
    rows, n = d // 16, sum(cols) // d
    vmem = lambda *shape: pltpu.VMEM((n, *shape, rows, d), BF)
    dma = lambda *shape: pltpu.SemaphoreType.DMA(shape)
    return pl.pallas_call(
        functools.partial(_sum_kernel, cols=cols), name="scatter_sums",
        in_specs=[pl.BlockSpec(memory_space=pl.ANY)] * len(grads), out_specs=pl.BlockSpec(memory_space=pl.ANY),
        out_shape=jax.ShapeDtypeStruct((rows, n * d), BF),
        scratch_shapes=[vmem(8), vmem(8), vmem(2, 4), vmem(4), vmem(4), vmem(4), pltpu.VMEM((n, rows, d), BF),
                        dma(n), dma(n), dma(n), dma(n), dma(n), dma(n, 3), dma(n, 4), dma(n)],
        compiler_params=pltpu.CompilerParams(collective_id=2, has_side_effects=True, vmem_limit_bytes=48 * MiB),
        cost_estimate=_cost(MiB, n * d * d),
    )(*[g.reshape(8, 2, rows, g.shape[1]) for g in grads])


def _factor_kernel(*refs, count):
    *ins, out_ref, got, send, recv = refs
    me = lax.axis_index("dp")
    others = [(me + k) % 16 for k in range(1, 16)]
    _greet(others)
    part = jnp.zeros(out_ref.shape, F32)
    for ref in ins:
        wide = jnp.square(ref[...].astype(F32))
        tall = sum(wide[i : i + 8] for i in range(0, wide.shape[0], 8))
        part += sum(tall[:, s] for s in _heads(wide.shape[1]))
    got[me] = part
    sent = [_remote(got.at[me], got.at[me], send.at[n], recv.at[me], to) for n, to in enumerate(others)]
    for one in sent:
        one.start()
    for to in others:
        _remote(got.at[to], got.at[to], send.at[0], recv.at[to], to).wait_recv()
    squares = jnp.sum(got[...].sum(0), keepdims=True)
    out_ref[...] = jnp.broadcast_to(jnp.minimum(1.0, 0.5 * lax.rsqrt(squares / count + 1e-30)), out_ref.shape)
    for one in sent:
        one.wait_send()


def clip_factor(blocks, count):
    shape = (8, HEAD)
    vmem = pl.BlockSpec(memory_space=pltpu.VMEM)
    return pl.pallas_call(
        functools.partial(_factor_kernel, count=count), name="clip_factor",
        in_specs=[vmem] * len(blocks), out_specs=vmem, out_shape=jax.ShapeDtypeStruct(shape, F32),
        scratch_shapes=[pltpu.VMEM((16, *shape), F32), pltpu.SemaphoreType.DMA((15,)), pltpu.SemaphoreType.DMA((16,))],
        compiler_params=pltpu.CompilerParams(collective_id=3, has_side_effects=True, vmem_limit_bytes=32 * MiB),
        cost_estimate=_cost(MiB, MiB),
    )(*blocks)


def adamw(w, m, v, g):
    m = 0.9 * m + 0.1 * g
    v = 0.95 * v + 0.05 * g * g
    step = m * lax.rsqrt(v + 1e-8) + 0.1 * w
    return (w - 0.02 * step).astype(BF), m, v


def sideways(w):
    rows = w.shape[0] // 4
    return w.reshape(4, rows, -1).transpose(1, 0, 2).reshape(rows, -1)


def upright(w):
    rows, d = w.shape[0], w.shape[1] // 4
    return w.reshape(rows, 4, d).transpose(1, 0, 2).reshape(4 * rows, d)


def solution(mesh):
    def step(x, dy, *arrays):
        weights, m, v = (arrays[i : i + 7] for i in (0, 7, 14))
        t, d = x.shape[1], x.shape[2]
        half = HEAD // 2
        angle = jnp.arange(t, dtype=F32)[:, None] * THETA ** (-jnp.arange(half, dtype=F32) / half)
        cos, sin = jnp.cos(angle), jnp.sin(angle)
        cos, sin = jnp.concatenate([cos, cos], 1), jnp.concatenate([-sin, sin], 1)

        def gathered(parts):
            return lax.all_gather(jnp.concatenate(parts, axis=1), "dp", axis=0, tiled=True)

        first, second = ([w[number] for w in weights] for number in range(2))
        head = gather_rows(jnp.concatenate(first[:3], axis=1))
        ffn = lambda one: [*one[4:6], sideways(one[6])]
        rest = gathered([*ffn(first), *ffn(second), *second[:4], first[3]])
        GATE, QKV, WO = (0, 12), (0, 24), (28, 27)

        h0 = x[0]
        qkv0 = qkv_forward(h0, head, 0, cos, sin)
        o0, lse0 = attend(qkv0)
        mid0, gate0, up0, h1 = ffn_forward(o0, h0, rest, WO[0], GATE[0])
        qkv1 = qkv_forward(h1, rest, QKV[1], cos, sin)
        o1, lse1 = attend(qkv1)
        by_mid1, ffn1 = ffn_backward(dy[0], rest, GATE[1], fresh=(o1, h1), wo_at=WO[1])

        def scattered(g):
            return lax.psum_scatter(g, "dp", scatter_dimension=0, tiled=True)

        got_ffn1 = scattered(ffn1)
        dq1, dk1, dv1, dwo1 = attend_backward(qkv1, o1, lse1, by_mid1, rest, WO[1])
        dqkv1, by_h1 = qkv_backward(dq1, dk1, dv1, h1, cos, sin, rest, QKV[1], by_mid1)
        by_mid0, ffn0 = ffn_backward(by_h1, rest, GATE[0], kept=(mid0, gate0, up0))
        got_ffn0 = scattered(ffn0)
        dq0, dk0, dv0, dwo0 = attend_backward(qkv0, o0, lse0, by_mid0, rest, WO[0])
        (dqkv0,) = qkv_backward(dq0, dk0, dv0, h0, cos, sin)
        got_attn = scatter_sums([dqkv1, dwo1, dqkv0, dwo0])
        got_attn1, got_attn0 = got_attn[:, : 4 * d], got_attn[:, 4 * d :]

        got = [[got_attn0, got_ffn0], [got_attn1, got_ffn1]]
        count = mesh.shape["dp"] * sum(w.size for w in weights)
        factor = clip_factor([got_attn, got_ffn1, got_ffn0], count)[0, 0]

        def gradient(number, name):
            attn, ffn = got[number]
            if name < 4:
                return attn[:, name * d : (name + 1) * d]
            part = ffn[:, (name - 4) * 4 * d : (name - 3) * 4 * d]
            return part if name < 6 else upright(part)

        new = []
        for name in range(7):
            g = jnp.stack([gradient(0, name), gradient(1, name)]).astype(F32) * factor
            new.append(adamw(weights[name].astype(F32), m[name], v[name], g))
        return tuple(one[which] for which in range(3) for one in new)

    states, cut = P(("rep", "dp"), None, None), P(None, "dp", None)
    return jax.shard_map(
        step,
        mesh=mesh,
        in_specs=(states, states) + (cut,) * 21,
        out_specs=(P("rep", "dp", None),) * 21,
        check_vma=False,
    )
```
